32 devices in a mesh: tm: 4 (over x, core), space: 8 (over z, y).
Axes of the slice: x: 2, y: 2, z: 4, core: 2. Of those that a mesh axis runs over, the one named last changes fastest.
Arguments:
- initial_state: float32 [512, 3, 512], P('space'), may hold values from -1 to 1, as said below
- applied_field: float32 [512, 3, 512], P('space'), may hold values from -2 to 2
- coupling: float32 [512, 512], P('space'), may hold values from 0.5 to 2
Outputs:
- slice_states: float32 [4, 512, 3, 512], P('tm', 'space')
The draws below stay inside these ranges and needn't reach their ends.
Inputs may be any that keep to these rules, and one draw needn't show every extreme that they name: `initial_state`: every cell's three components form a vector of length one.
All inputs are finite; a program needn't handle non-finite values.
Results may differ from the reference program's by a relative error of at most 0.00014.
Values sent between devices are 32-bit elements; how exact they have to be, the bound alone decides.
A program may use at most 128 MiB of HBM per device.

```python
import math
import jax
import jax.numpy as jnp

GRID = 512
FINE = 2
ITERS = 1
SLICES = 4


def base_frame(key):
    frame_key = jax.random.fold_in(key, 7)
    sign_key, tilt_key = jax.random.split(frame_key)
    signs = (2 * jax.random.randint(sign_key, (3,), 0, 2) - 1).astype(jnp.float32)
    tilt = jax.random.uniform(tilt_key, (), jnp.float32, 0.6, 0.9)
    return (signs, tilt)


def draw_initial_state(key, part):
    signs, tilt = base_frame(key)
    noise_key = jax.random.fold_in(key, 11)
    in_plane = jnp.cos(tilt) / math.sqrt(2.0)
    base = jnp.stack([signs[0] * in_plane, signs[1] * in_plane, signs[2] * jnp.sin(tilt)]).reshape(1, 3, 1)
    noise = jax.random.uniform(noise_key, (GRID, 3, GRID), jnp.float32, -0.45, 0.45)
    vector = base + noise
    length = jnp.sqrt(jnp.sum(vector * vector, axis=1, keepdims=True))
    return vector / length


def draw_applied_field(key, part):
    signs, tilt = base_frame(key)
    noise_key = jax.random.fold_in(key, 13)
    field_scale = 2.5 / math.sqrt(2.0)
    base = jnp.stack([-signs[1] * field_scale, signs[0] * field_scale, 0.0 * field_scale]).reshape(1, 3, 1)
    noise = 0.4 * jax.random.normal(noise_key, (GRID, 3, GRID), jnp.float32)
    return jnp.clip(base + noise, -2.0, 2.0)


def shard_levels(rng, dims, cuts, low, top_value):
    def one(dim, blocks):
        steps = jax.random.uniform(jax.random.fold_in(jax.random.fold_in(rng, 6), dim), (blocks,), jnp.float32, low / len(cuts), top_value / len(cuts))
        return jnp.repeat(jnp.exp(steps), dims[dim] // blocks).reshape((-1,) + (1,) * (len(dims) - dim - 1))

    gain = one(*cuts[0])
    for cut in cuts[1:]:
        gain = gain * one(*cut)
    return gain


def setup_inputs(seed: int = 0) -> dict:
    arg_keys = jax.random.split(jax.random.key(seed), 4)
    initial_state = draw_initial_state(jax.random.fold_in(arg_keys[3], 71), 0)
    applied_field = draw_applied_field(jax.random.fold_in(arg_keys[3], 71), 0)
    coupling = jnp.clip(jnp.exp(math.log(2.0) - 1.3862944 * jax.random.uniform(arg_keys[2], (GRID, GRID), jnp.float32) ** shard_levels(arg_keys[2], (GRID, GRID), ((0, 8),), -0.2, 0.2)), 0.5, 2.0)
    return dict(initial_state=initial_state, applied_field=applied_field, coupling=coupling)


step_time = 0.06
damping = 0.02
stiffness = 0.25
thickness = 8.0

def spectral_tensor(row_index, column_index, length):
    half_length = length // 2
    signed_rows = jnp.where(row_index < half_length, row_index, row_index - length).astype(jnp.float32)
    signed_columns = jnp.where(column_index < half_length, column_index, column_index - length).astype(jnp.float32)
    wave_rows = 2.0 * math.pi / length * signed_rows[:, None]
    wave_columns = 2.0 * math.pi / length * signed_columns[None, :]
    squared = wave_rows * wave_rows + wave_columns * wave_columns
    nonzero = squared > 0.0
    safe_square = jnp.where(nonzero, squared, 1.0)
    scaled_wave = jnp.sqrt(safe_square) * thickness
    film_factor = jnp.where(nonzero, (1.0 - jnp.exp(-scaled_wave)) / scaled_wave, 1.0)
    in_plane = (1.0 - film_factor) / safe_square
    nyquist = (row_index[:, None] == half_length) | (column_index[None, :] == half_length)
    normalizer = -1.0 / (length * length)
    tensor_first = in_plane * wave_columns * wave_columns * normalizer
    tensor_second = in_plane * wave_rows * wave_rows * normalizer
    tensor_cross = jnp.where(nyquist, 0.0, in_plane * wave_columns * wave_rows) * normalizer
    tensor_normal = film_factor * normalizer
    return (tensor_first, tensor_second, tensor_cross, tensor_normal)

def exchange_field(padded_state, padded_coupling):
    center_state = padded_state[1:-1]
    center_coupling = padded_coupling[1:-1]
    wide_state = jnp.pad(padded_state, ((0, 0), (0, 0), (1, 1)))
    wide_coupling = jnp.pad(padded_coupling, ((0, 0), (1, 1)))
    neighbour_sum = padded_coupling[2:, None, :] * (padded_state[2:] - center_state)
    neighbour_sum = neighbour_sum + padded_coupling[:-2, None, :] * (padded_state[:-2] - center_state)
    neighbour_sum = neighbour_sum + wide_coupling[1:-1, None, 2:] * (wide_state[1:-1, :, 2:] - center_state)
    neighbour_sum = neighbour_sum + wide_coupling[1:-1, None, :-2] * (wide_state[1:-1, :, :-2] - center_state)
    return stiffness * center_coupling[:, None, :] * neighbour_sum

def torque(magnet, effective):
    first_cross = jnp.cross(magnet, effective, axis=1)
    second_cross = jnp.cross(magnet, first_cross, axis=1)
    return -(first_cross + damping * second_cross) / (1.0 + damping * damping)

def demag_field(magnet):
    padded = jnp.pad(magnet, ((0, GRID), (0, 0), (0, GRID)))
    spectrum = jnp.fft.fft2(padded, axes=(0, 2))
    index_all = jnp.arange(2 * GRID, dtype=jnp.int32)
    tensor_first, tensor_second, tensor_cross, tensor_normal = spectral_tensor(index_all, index_all, 2 * GRID)
    first_out = tensor_first * spectrum[:, 0] + tensor_cross * spectrum[:, 1]
    second_out = tensor_cross * spectrum[:, 0] + tensor_second * spectrum[:, 1]
    third_out = tensor_normal * spectrum[:, 2]
    combined = jnp.stack([first_out, second_out, third_out], axis=1)
    result = jnp.fft.ifft2(combined, axes=(0, 2)) * float(2 * GRID * (2 * GRID))
    return jnp.real(result)[:GRID, :, :GRID].astype(jnp.float32)

def effective_fine(magnet, applied_field, padded_coupling):
    padded_state = jnp.pad(magnet, ((1, 1), (0, 0), (0, 0)))
    return exchange_field(padded_state, padded_coupling) + demag_field(magnet) + applied_field

def propagate_fine(magnet, applied_field, padded_coupling):
    for repeat in range(FINE):
        first_rate = torque(magnet, effective_fine(magnet, applied_field, padded_coupling))
        predicted = magnet + step_time * first_rate
        second_rate = torque(predicted, effective_fine(predicted, applied_field, padded_coupling))
        magnet = magnet + 0.5 * step_time * (first_rate + second_rate)
    return magnet

def propagate_coarse(magnet, applied_field, padded_coupling):
    padded_state = jnp.pad(magnet, ((1, 1), (0, 0), (0, 0)))
    local_demag = jnp.array([0.0, 0.0, -1.0], dtype=jnp.float32).reshape(1, 3, 1)
    effective = exchange_field(padded_state, padded_coupling) + applied_field + magnet * local_demag
    return magnet + FINE * step_time * torque(magnet, effective)

def coarse_sweep(differences, initial_state, applied_field, padded_coupling):
    current = initial_state
    starts = []
    coarse_ends = []
    slice_ends = []
    for slice_number in range(SLICES):
        predicted = propagate_coarse(current, applied_field, padded_coupling)
        advanced = predicted + differences[slice_number]
        starts.append(current)
        coarse_ends.append(predicted)
        slice_ends.append(advanced)
        current = advanced
    return (starts, coarse_ends, slice_ends)

def reference(initial_state, applied_field, coupling):
    padded_coupling = jnp.pad(coupling, ((1, 1), (0, 0)))
    differences = [jnp.zeros_like(initial_state) for slice_number in range(SLICES)]
    starts, coarse_ends, slice_ends = coarse_sweep(differences, initial_state, applied_field, padded_coupling)
    for iteration in range(ITERS):
        differences = [propagate_fine(starts[slice_number], applied_field, padded_coupling) - coarse_ends[slice_number] for slice_number in range(SLICES)]
        starts, coarse_ends, slice_ends = coarse_sweep(differences, initial_state, applied_field, padded_coupling)
    return jnp.stack(slice_ends, axis=0)
```

```python
import math

import jax
import jax.numpy as jnp
import numpy as np
from jax import lax
from jax.sharding import Mesh, PartitionSpec as P

FINE = 2
step_time = 0.06
damping = 0.02
stiffness = 0.25
thickness = 8.0

RING = ("core", "rest")
LOCAL = ("core", "zh", "rest")
EVERY = ("x", "core", "zh", "rest")


def real_tables(grid, parts):
    length = 2 * grid
    place = np.arange(grid)
    wave = np.arange(grid)
    angle = 2.0 * np.pi / length * ((place[:, None] * wave[None, :]) % length)
    cosine, sine = np.cos(angle), np.sin(angle)
    sine[:, 0] = 1.0 - 2.0 * (place % 2)
    width = grid // parts
    tall = np.concatenate([cosine, sine], axis=1).astype(np.float32)
    blocks = np.stack([cosine.reshape(grid, parts, width), sine.reshape(grid, parts, width)], axis=2)
    return tall, blocks.reshape(grid, length).astype(np.float32)


def spectral_tensor(rows, columns, length):
    wave_rows = 2.0 * math.pi / length * rows.astype(jnp.float32)
    wave_columns = 2.0 * math.pi / length * columns.astype(jnp.float32)
    squared = wave_rows * wave_rows + wave_columns * wave_columns
    nonzero = squared > 0.0
    safe = jnp.where(nonzero, squared, 1.0)
    scaled = jnp.sqrt(safe) * thickness
    film = jnp.where(nonzero, (1.0 - jnp.exp(-scaled)) / scaled, 1.0)
    in_plane = (1.0 - film) / safe
    half = length // 2
    edge_row = (rows == 0) | (rows == half)
    edge_column = (columns == 0) | (columns == half)
    weight = jnp.where(edge_row, 1.0, 2.0) * jnp.where(edge_column, 1.0, 2.0) * (-1.0 / (length * length))
    return (
        in_plane * wave_columns * wave_columns * weight,
        in_plane * wave_rows * wave_rows * weight,
        jnp.where(edge_row | edge_column, 0.0, in_plane * wave_columns * wave_rows * weight),
        film * weight,
    )


def exchange_field(padded, pad_coupling):
    center = padded[:, 1:-1]
    coupling = pad_coupling[1:-1]
    wide = jnp.pad(padded[:, 1:-1], ((0, 0), (0, 0), (1, 1)))
    wide_coupling = jnp.pad(coupling, ((0, 0), (1, 1)))
    total = pad_coupling[2:] * (padded[:, 2:] - center)
    total = total + pad_coupling[:-2] * (padded[:, :-2] - center)
    total = total + wide_coupling[:, 2:] * (wide[:, :, 2:] - center)
    total = total + wide_coupling[:, :-2] * (wide[:, :, :-2] - center)
    return stiffness * coupling * total


def cross(a, b):
    return jnp.stack([a[1] * b[2] - a[2] * b[1], a[2] * b[0] - a[0] * b[2], a[0] * b[1] - a[1] * b[0]])


def torque(magnet, effective):
    first = cross(magnet, effective)
    return -(first + damping * cross(magnet, first)) * (1.0 / (1.0 + damping * damping))


def coarse(padded, pad_coupling, field):
    center = padded[:, 1:-1]
    effective = exchange_field(padded, pad_coupling) + field
    effective = jnp.stack([effective[0], effective[1], effective[2] - center[2]])
    return center + FINE * step_time * torque(center, effective)


def dot(left, right):
    return jnp.dot(left, right, precision=lax.Precision.HIGH)


def make_shards(tm, space):
    rest = space // 2

    def swapped(role):
        core, zh, r = role // space, role // rest % 2, role % rest
        return zh * space + core * rest + r

    def shards(initial_state, applied_field, coupling):
        rows, _, grid = initial_state.shape
        length = 2 * grid
        width = length // space
        depth = tm
        part = lax.axis_index(RING)
        old_slice = lax.axis_index(("x", "core"))
        new_slice = lax.axis_index(("x", "zh"))
        tall, blocks = real_tables(grid, space)

        start = jnp.transpose(initial_state, (1, 0, 2))
        field = jnp.transpose(applied_field, (1, 0, 2))
        pack = jnp.concatenate([start, field, coupling[None]], axis=0)

        def fetch(block, shift):
            pairs = []
            for device in range(2 * space):
                core, zh, r = device // space, device // rest % 2, device % rest
                wanted = core * rest + r + shift
                if 0 <= wanted < space:
                    pairs.append((zh * space + wanted, device))
            return lax.ppermute(block, LOCAL, pairs)

        middle = fetch(pack, 0)
        before = fetch(pack[:, rows - depth :], -1)
        after = fetch(pack[:, :depth], 1)
        wide = jnp.concatenate([before, middle, after], axis=1)
        wide_coupling = wide[6]
        wide_field = wide[3:6]
        state = wide[:3]
        fine_start, coarse_end = state, state
        for n in range(tm):
            stepped = jnp.pad(
                coarse(state, wide_coupling, wide_field[:, 1:-1]), ((0, 0), (1, 1), (0, 0))
            )
            here = new_slice == n
            fine_start = jnp.where(here, state, fine_start)
            coarse_end = jnp.where(here, stepped, coarse_end)
            state = stepped
        fine_field = wide_field[:, depth:-depth]
        fine_coupling = wide_coupling[depth - 1 : rows + depth + 1]
        coarse_end = coarse_end[:, depth:-depth]

        slot = jnp.arange(length, dtype=jnp.int32)
        wave_y = jnp.where(slot == grid, grid, slot % grid)
        lane = jnp.arange(width, dtype=jnp.int32)
        wave_x = part * (width // 2) + lane % (width // 2)
        wave_x = jnp.where((wave_x == 0) & (lane >= width // 2), grid, wave_x)
        txx, tyy, txy, tzz = spectral_tensor(wave_y[:, None], wave_x[None, :], length)
        same = ((slot >= grid)[:, None]) == ((lane >= width // 2)[None, :])
        txy = jnp.where(same, -txy, txy)

        def partner(values):
            values = jnp.concatenate([values[grid:], values[:grid]], axis=0)
            return jnp.concatenate([values[:, width // 2 :], values[:, : width // 2]], axis=1)

        edge_rows = 6 * grid // width
        has_before = part > 0
        has_after = part < space - 1

        def fine_field_of(magnet):
            coefs = dot(magnet.reshape(3 * rows, grid), blocks)
            edges = jnp.concatenate([magnet[:, :1], magnet[:, -1:]], axis=1).reshape(edge_rows, width)
            payload = jnp.transpose(coefs.reshape(3 * rows, space, width), (1, 0, 2))
            payload = jnp.concatenate(
                [payload, jnp.broadcast_to(edges[None], (space, edge_rows, width))], axis=1
            )
            got = lax.all_to_all(payload, RING, split_axis=0, concat_axis=0, tiled=True)
            columns = jnp.concatenate(
                [got[:, c * rows : (c + 1) * rows].reshape(grid, width) for c in range(3)], axis=1
            )
            spectrum = dot(tall.T, columns)
            sx, sy, sz = (spectrum[:, c * width : (c + 1) * width] for c in range(3))
            mixed = jnp.concatenate(
                [txx * sx + txy * partner(sy), txy * partner(sx) + tyy * sy, tzz * sz], axis=1
            )
            back = dot(tall, mixed).reshape(space, rows, 3 * width)
            back = lax.all_to_all(back, RING, split_axis=0, concat_axis=0, tiled=True)
            back = jnp.transpose(back.reshape(space, rows, 3, width), (2, 1, 0, 3)).reshape(3 * rows, length)
            demag = dot(back, blocks.T).reshape(3, rows, grid)

            def edge_of(shift, which, there):
                index = jnp.clip(part + shift, 0, space - 1)
                taken = lax.dynamic_slice_in_dim(got, index, 1, 0)[0, 3 * rows :]
                taken = taken.reshape(3, 2, grid)[:, which : which + 1]
                return jnp.where(there, taken, 0.0)

            padded = jnp.concatenate(
                [edge_of(-1, 1, has_before), magnet, edge_of(1, 0, has_after)], axis=1
            )
            return exchange_field(padded, fine_coupling) + demag + fine_field

        magnet = fine_start[:, depth:-depth]
        for repeat in range(FINE):
            first_rate = torque(magnet, fine_field_of(magnet))
            predicted = magnet + step_time * first_rate
            second_rate = torque(predicted, fine_field_of(predicted))
            magnet = magnet + 0.5 * step_time * (first_rate + second_rate)
        jump = magnet - coarse_end
        jump = lax.ppermute(jump, LOCAL, [(swapped(i), i) for i in range(2 * space)])

        def along(block, slice_shift, row_shift):
            pairs = []
            for device in range(tm * space):
                n, s = device // space - slice_shift, device % space + row_shift
                if 0 <= n and 0 <= s < space:
                    pairs.append((n * space + s, device))
            return lax.ppermute(block, EVERY, pairs)

        def padded_from(block, slice_shift, with_middle):
            up = along(block[:, -1:], slice_shift, -1)
            down = along(block[:, :1], slice_shift, 1)
            middle = along(block[:3], slice_shift, 0) if with_middle else block
            return jnp.concatenate([up, middle, down], axis=1)

        home = padded_from(jnp.concatenate([start, coupling[None]], axis=0), 0, False)
        home_state, home_coupling = home[:3], home[3]
        end = coarse(home_state, home_coupling, field) + jump
        for n in range(1, tm):
            current = jnp.where(old_slice == 0, home_state, padded_from(end, 1, True))
            end = coarse(current, home_coupling, field) + jump
        return jnp.transpose(end, (1, 0, 2))[None]

    return shards


def solution(mesh):
    tm, space = mesh.shape["tm"], mesh.shape["space"]
    finer = Mesh(mesh.devices.reshape(tm // 2, 2, 2, space // 2), EVERY)
    rows = ("zh", "rest")
    return jax.shard_map(
        make_shards(tm, space),
        mesh=finer,
        in_specs=(P(rows, None, None), P(rows, None, None), P(rows, None)),
        out_specs=P(("x", "core"), rows, None, None),
        check_vma=False,
    )
```

```python
import math

import jax
import jax.numpy as jnp
import numpy as np
from jax import lax
from jax.experimental import pallas as pl
from jax.experimental.pallas import tpu as pltpu
from jax.sharding import Mesh, PartitionSpec as P

FINE = 2
step_time = 0.06
damping = 0.02
stiffness = 0.25
thickness = 8.0

RING = ("core", "rest")
LOCAL = ("core", "zh", "rest")
EVERY = ("x", "core", "zh", "rest")


def real_tables(grid, parts):
    length = 2 * grid
    place = np.arange(grid)
    wave = np.arange(grid)
    angle = 2.0 * np.pi / length * ((place[:, None] * wave[None, :]) % length)
    cosine, sine = np.cos(angle), np.sin(angle)
    sine[:, 0] = 1.0 - 2.0 * (place % 2)
    width = grid // parts
    tall = np.concatenate([cosine, sine], axis=1).astype(np.float32)
    blocks = np.stack([cosine.reshape(grid, parts, width), sine.reshape(grid, parts, width)], axis=2)
    return tall, blocks.reshape(grid, length).astype(np.float32)


def spectral_tensor(rows, columns, length):
    wave_rows = 2.0 * math.pi / length * rows.astype(jnp.float32)
    wave_columns = 2.0 * math.pi / length * columns.astype(jnp.float32)
    squared = wave_rows * wave_rows + wave_columns * wave_columns
    nonzero = squared > 0.0
    safe = jnp.where(nonzero, squared, 1.0)
    scaled = jnp.sqrt(safe) * thickness
    film = jnp.where(nonzero, (1.0 - jnp.exp(-scaled)) / scaled, 1.0)
    in_plane = (1.0 - film) / safe
    half = length // 2
    edge_row = (rows == 0) | (rows == half)
    edge_column = (columns == 0) | (columns == half)
    weight = jnp.where(edge_row, 1.0, 2.0) * jnp.where(edge_column, 1.0, 2.0) * (-1.0 / (length * length))
    return (
        in_plane * wave_columns * wave_columns * weight,
        in_plane * wave_rows * wave_rows * weight,
        jnp.where(edge_row | edge_column, 0.0, in_plane * wave_columns * wave_rows * weight),
        film * weight,
    )


def exchange_field(padded, pad_coupling):
    center = padded[:, 1:-1]
    coupling = pad_coupling[1:-1]
    wide = jnp.pad(padded[:, 1:-1], ((0, 0), (0, 0), (1, 1)))
    wide_coupling = jnp.pad(coupling, ((0, 0), (1, 1)))
    total = pad_coupling[2:] * (padded[:, 2:] - center)
    total = total + pad_coupling[:-2] * (padded[:, :-2] - center)
    total = total + wide_coupling[:, 2:] * (wide[:, :, 2:] - center)
    total = total + wide_coupling[:, :-2] * (wide[:, :, :-2] - center)
    return stiffness * coupling * total


def cross(a, b):
    return jnp.stack([a[1] * b[2] - a[2] * b[1], a[2] * b[0] - a[0] * b[2], a[0] * b[1] - a[1] * b[0]])


def torque(magnet, effective):
    first = cross(magnet, effective)
    return -(first + damping * cross(magnet, first)) * (1.0 / (1.0 + damping * damping))


def coarse(padded, pad_coupling, field):
    center = padded[:, 1:-1]
    effective = exchange_field(padded, pad_coupling) + field
    effective = jnp.stack([effective[0], effective[1], effective[2] - center[2]])
    return center + FINE * step_time * torque(center, effective)


def dot(left, right):
    return jnp.dot(left, right, precision=lax.Precision.HIGH)


def halves(table):
    high = table.astype(jnp.bfloat16)
    return [high, (table - high.astype(np.float32)).astype(jnp.bfloat16)]


def split(value):
    high = value.astype(jnp.bfloat16)
    return high, (value - high.astype(jnp.float32)).astype(jnp.bfloat16)


def dot3(left_high, left_low, right_high, right_low):
    def one(a, b):
        return jnp.dot(a, b, preferred_element_type=jnp.float32)

    return one(left_high, right_high) + (one(left_high, right_low) + one(left_low, right_high))


def fine_kernel(
    space,
    start, field, links, coarse_end, tensors,
    cut_high, cut_low, up_high, up_low, tall_high, tall_low, back_high, back_low,
    out,
    current, rate, base, edge_out, edge_in, send, got, send_back, got_back,
    columns_high, columns_low, mixed_high, mixed_low, wide_high, wide_low, demag,
    edge_sems, send_sems, got_sems, send_back_sems, got_back_sems,
):
    _, rows, grid = start.shape
    rest = space // 2
    width = 2 * grid // space
    part = lax.axis_index("core") * rest + lax.axis_index("rest")

    def device(target):
        return {"core": target // rest, "rest": target % rest}

    barrier = pltpu.get_barrier_semaphore()

    def greet(k, carry):
        pl.semaphore_signal(
            barrier, inc=1, device_id=device((part + k) % space), device_id_type=pl.DeviceIdType.MESH
        )
        return carry

    lax.fori_loop(1, space, greet, 0)
    pl.semaphore_wait(barrier, space - 1)

    def remote(source, target, send_sem, recv_sem, where):
        return pltpu.make_async_remote_copy(
            src_ref=source, dst_ref=target, send_sem=send_sem, recv_sem=recv_sem,
            device_id=device(where), device_id_type=pl.DeviceIdType.MESH,
        )

    def forward(k):
        target = (part + k) % space
        return remote(send.at[target], got.at[part], send_sems.at[k], got_sems.at[k], target)

    def backward(k):
        target = (part + k) % space
        return remote(
            send_back.at[target], got_back.at[part], send_back_sems.at[k], got_back_sems.at[k], target
        )

    current[:, 8 : 8 + rows, :] = start[...]
    base[...] = start[...]

    def evaluate(parity):
        for c in range(3):
            edge_out[0, c : c + 1, :] = current[c, 8:9, :]
            edge_out[1, c : c + 1, :] = current[c, 7 + rows : 8 + rows, :]
        magnet_high, magnet_low = split(current[:, 8 : 8 + rows, :].reshape(3 * rows, grid))
        wide_high[:, :grid] = magnet_high
        wide_low[:, :grid] = magnet_low

        def block(index):
            return dot3(wide_high[:, :grid], wide_low[:, :grid], cut_high[index], cut_low[index])

        to_before = remote(
            edge_out.at[0], edge_in.at[parity, 1], edge_sems.at[0], edge_sems.at[1], (part + space - 1) % space
        )
        to_after = remote(
            edge_out.at[1], edge_in.at[parity, 0], edge_sems.at[2], edge_sems.at[3], (part + 1) % space
        )
        to_before.start()
        to_after.start()

        def push(k, carry):
            target = (part + k) % space
            send[target] = block(target)
            forward(k).start()
            return carry

        lax.fori_loop(1, space, push, 0)
        got[part] = block(part)

        def take(k, carry):
            forward(k).wait()
            return carry

        lax.fori_loop(1, space, take, 0)
        to_before.wait()
        to_after.wait()
        for c in range(3):
            current[c, 7:8, :] = edge_in[parity, 0, c : c + 1, :]
            current[c, 8 + rows : 9 + rows, :] = edge_in[parity, 1, c : c + 1, :]
        columns = jnp.concatenate(
            [got[:, c * rows : (c + 1) * rows, :].reshape(grid, width) for c in range(3)], axis=1
        )
        columns_high[...], columns_low[...] = split(columns)

        step = grid // 2

        def mix(i, carry):
            lower = pl.multiple_of(i * step, step)
            upper = pl.multiple_of(grid + i * step, step)

            def spectrum(at):
                return dot3(
                    up_high[pl.ds(at, step), :], up_low[pl.ds(at, step), :], columns_high[...], columns_low[...]
                )

            pair = (spectrum(lower), spectrum(upper))
            for q, at in enumerate((lower, upper)):
                txx, tyy, txy, tzz = (tensors[n, pl.ds(at, step), :] for n in range(4))
                sx, sy, sz = (pair[q][:, c * width : (c + 1) * width] for c in range(3))
                ox, oy = (pltpu.roll(pair[1 - q][:, c * width : (c + 1) * width], width // 2, 1) for c in range(2))
                for c, value in enumerate((txx * sx + txy * oy, txy * ox + tyy * sy, tzz * sz)):
                    high, low = split(value)
                    mixed_high[pl.ds(at, step), c * width : (c + 1) * width] = high
                    mixed_low[pl.ds(at, step), c * width : (c + 1) * width] = low
            return carry

        lax.fori_loop(0, 2, mix, 0)

        def synth(i, carry):
            at = pl.multiple_of(i * step, step)
            value = dot3(
                tall_high[pl.ds(at, step), :], tall_low[pl.ds(at, step), :], mixed_high[...], mixed_low[...]
            )
            send_back[pl.ds(i * (space // 2), space // 2)] = value.reshape(space // 2, rows, 3 * width)
            return carry

        lax.fori_loop(0, 2, synth, 0)

        def push_back(k, carry):
            backward(k).start()
            return carry

        lax.fori_loop(1, space, push_back, 0)
        got_back[part] = send_back[part]

        def take_back(k, carry):
            backward(k).wait()
            return carry

        lax.fori_loop(1, space, take_back, 0)
        for j in range(space):
            for c in range(3):
                high, low = split(got_back[j, :, c * width : (c + 1) * width])
                wide_high[c * rows : (c + 1) * rows, j * width : (j + 1) * width] = high
                wide_low[c * rows : (c + 1) * rows, j * width : (j + 1) * width] = low
        demag[...] = dot3(wide_high[...], wide_low[...], back_high[...], back_low[...])

        for at in range(0, rows, 8):
            inside = [current[c, 8 + at : 16 + at, :] for c in range(3)]
            weights = [links[n, at : at + 8, :] for n in range(4)]
            effective = []
            for c in range(3):
                m = inside[c]
                total = weights[0] * (current[c, 7 + at : 15 + at, :] - m)
                total = total + weights[1] * (current[c, 9 + at : 17 + at, :] - m)
                total = total + weights[2] * (pltpu.roll(m, 1, 1) - m)
                total = total + weights[3] * (pltpu.roll(m, grid - 1, 1) - m)
                effective.append(total + demag[c * rows + at : c * rows + at + 8, :] + field[c, at : at + 8, :])
            first = cross_of(inside, effective)
            second = cross_of(inside, first)
            for c in range(3):
                value = -(first[c] + damping * second[c]) * (1.0 / (1.0 + damping * damping))
                if parity == 0:
                    rate[c, at : at + 8, :] = value
                else:
                    moved = base[c, at : at + 8, :] + 0.5 * step_time * (rate[c, at : at + 8, :] + value)
                    base[c, at : at + 8, :] = moved
        if parity == 0:
            current[:, 8 : 8 + rows, :] = base[...] + step_time * rate[...]
        else:
            current[:, 8 : 8 + rows, :] = base[...]

    def fine_step(i, carry):
        evaluate(0)
        evaluate(1)
        return carry

    lax.fori_loop(0, FINE, fine_step, 0)
    out[...] = base[...] - coarse_end[...]


def cross_of(a, b):
    return [a[1] * b[2] - a[2] * b[1], a[2] * b[0] - a[0] * b[2], a[0] * b[1] - a[1] * b[0]]


def fine_jump(space, start, field, links, coarse_end, tensors, tables):
    _, rows, grid = start.shape
    length = 2 * grid
    width = length // space

    def kernel(*refs):
        fine_kernel(space, *refs)

    f32, bf16 = jnp.float32, jnp.bfloat16
    operands = [start, field, links, coarse_end, tensors, *tables]
    return pl.pallas_call(
        kernel,
        out_shape=jax.ShapeDtypeStruct(start.shape, f32),
        in_specs=[pl.BlockSpec(memory_space=pltpu.VMEM)] * len(operands),
        out_specs=pl.BlockSpec(memory_space=pltpu.VMEM),
        scratch_shapes=[
            pltpu.VMEM((3, rows + 16, grid), f32),
            pltpu.VMEM((3, rows, grid), f32),
            pltpu.VMEM((3, rows, grid), f32),
            pltpu.VMEM((2, 8, grid), f32),
            pltpu.VMEM((2, 2, 8, grid), f32),
            pltpu.VMEM((space, 3 * rows, width), f32),
            pltpu.VMEM((space, 3 * rows, width), f32),
            pltpu.VMEM((space, rows, 3 * width), f32),
            pltpu.VMEM((space, rows, 3 * width), f32),
            pltpu.VMEM((grid, 3 * width), bf16),
            pltpu.VMEM((grid, 3 * width), bf16),
            pltpu.VMEM((length, 3 * width), bf16),
            pltpu.VMEM((length, 3 * width), bf16),
            pltpu.VMEM((3 * rows, length), bf16),
            pltpu.VMEM((3 * rows, length), bf16),
            pltpu.VMEM((3 * rows, grid), f32),
            pltpu.SemaphoreType.DMA((4,)),
            pltpu.SemaphoreType.DMA((space,)),
            pltpu.SemaphoreType.DMA((space,)),
            pltpu.SemaphoreType.DMA((space,)),
            pltpu.SemaphoreType.DMA((space,)),
        ],
        compiler_params=pltpu.CompilerParams(
            collective_id=0, has_side_effects=True, vmem_limit_bytes=56 * 1024 * 1024
        ),
    )(*operands)


def make_shards(tm, space):
    rest = space // 2

    def swapped(role):
        core, zh, r = role // space, role // rest % 2, role % rest
        return zh * space + core * rest + r

    def shards(initial_state, applied_field, coupling):
        rows, _, grid = initial_state.shape
        length = 2 * grid
        width = length // space
        depth = tm
        part = lax.axis_index(RING)
        old_slice = lax.axis_index(("x", "core"))
        new_slice = lax.axis_index(("x", "zh"))
        tall, blocks = real_tables(grid, space)

        start = jnp.transpose(initial_state, (1, 0, 2))
        field = jnp.transpose(applied_field, (1, 0, 2))
        pack = jnp.concatenate([start, field, coupling[None]], axis=0)

        def fetch(block, shift):
            pairs = []
            for device in range(2 * space):
                core, zh, r = device // space, device // rest % 2, device % rest
                wanted = core * rest + r + shift
                if 0 <= wanted < space:
                    pairs.append((zh * space + wanted, device))
            return lax.ppermute(block, LOCAL, pairs)

        middle = fetch(pack, 0)
        before = fetch(pack[:, rows - depth :], -1)
        after = fetch(pack[:, :depth], 1)
        wide = jnp.concatenate([before, middle, after], axis=1)
        wide_coupling = wide[6]
        wide_field = wide[3:6]
        state = wide[:3]
        fine_start, coarse_end = state, state
        for n in range(tm):
            stepped = jnp.pad(
                coarse(state, wide_coupling, wide_field[:, 1:-1]), ((0, 0), (1, 1), (0, 0))
            )
            here = new_slice == n
            fine_start = jnp.where(here, state, fine_start)
            coarse_end = jnp.where(here, stepped, coarse_end)
            state = stepped
        fine_field = wide_field[:, depth:-depth]
        fine_coupling = wide_coupling[depth - 1 : rows + depth + 1]
        coarse_end = coarse_end[:, depth:-depth]

        slot = jnp.arange(length, dtype=jnp.int32)
        wave_y = jnp.where(slot == grid, grid, slot % grid)
        lane = jnp.arange(width, dtype=jnp.int32)
        wave_x = part * (width // 2) + lane % (width // 2)
        wave_x = jnp.where((wave_x == 0) & (lane >= width // 2), grid, wave_x)
        txx, tyy, txy, tzz = spectral_tensor(wave_y[:, None], wave_x[None, :], length)
        same = ((slot >= grid)[:, None]) == ((lane >= width // 2)[None, :])
        txy = jnp.where(same, -txy, txy)

        own = wide_coupling[depth : rows + depth]
        flat = jnp.pad(own, ((0, 0), (1, 1)))
        links = stiffness * own[None] * jnp.stack(
            [
                wide_coupling[depth - 1 : rows + depth - 1],
                wide_coupling[depth + 1 : rows + depth + 1],
                flat[:, :-2],
                flat[:, 2:],
            ]
        )
        cut = np.transpose(blocks.reshape(grid, space, width), (1, 0, 2))
        tables = [part_ for table in (cut, tall.T, tall, blocks.T) for part_ in halves(table)]
        jump = fine_jump(
            space, fine_start[:, depth:-depth], fine_field, links, coarse_end, jnp.stack([txx, tyy, txy, tzz]), tables
        )
        jump = lax.ppermute(jump, LOCAL, [(swapped(i), i) for i in range(2 * space)])

        def along(block, slice_shift, row_shift):
            pairs = []
            for device in range(tm * space):
                n, s = device // space - slice_shift, device % space + row_shift
                if 0 <= n and 0 <= s < space:
                    pairs.append((n * space + s, device))
            return lax.ppermute(block, EVERY, pairs)

        def padded_from(block, slice_shift, with_middle):
            up = along(block[:, -1:], slice_shift, -1)
            down = along(block[:, :1], slice_shift, 1)
            middle = along(block[:3], slice_shift, 0) if with_middle else block
            return jnp.concatenate([up, middle, down], axis=1)

        home = padded_from(jnp.concatenate([start, coupling[None]], axis=0), 0, False)
        home_state, home_coupling = home[:3], home[3]
        end = coarse(home_state, home_coupling, field) + jump
        for n in range(1, tm):
            current = jnp.where(old_slice == 0, home_state, padded_from(end, 1, True))
            end = coarse(current, home_coupling, field) + jump
        return jnp.transpose(end, (1, 0, 2))[None]

    return shards


def solution(mesh):
    tm, space = mesh.shape["tm"], mesh.shape["space"]
    finer = Mesh(mesh.devices.reshape(tm // 2, 2, 2, space // 2), EVERY)
    rows = ("zh", "rest")
    return jax.shard_map(
        make_shards(tm, space),
        mesh=finer,
        in_specs=(P(rows, None, None), P(rows, None, None), P(rows, None)),
        out_specs=P(("x", "core"), rows, None, None),
        check_vma=False,
    )
```

```python
import math

import jax
import jax.numpy as jnp
import numpy as np
from jax import lax
from jax.experimental import pallas as pl
from jax.experimental.pallas import tpu as pltpu
from jax.sharding import Mesh, PartitionSpec as P

FINE = 2
step_time = 0.06
damping = 0.02
stiffness = 0.25
thickness = 8.0

RING = ("core", "rest")
LOCAL = ("core", "zh", "rest")
EVERY = ("x", "core", "zh", "rest")


def real_tables(grid, parts):
    length = 2 * grid
    place = np.arange(grid)
    wave = np.arange(grid)
    angle = 2.0 * np.pi / length * ((place[:, None] * wave[None, :]) % length)
    cosine, sine = np.cos(angle), np.sin(angle)
    sine[:, 0] = 1.0 - 2.0 * (place % 2)
    width = grid // parts
    tall = np.concatenate([cosine, sine], axis=1).astype(np.float32)
    blocks = np.stack([cosine.reshape(grid, parts, width), sine.reshape(grid, parts, width)], axis=2)
    return tall, blocks.reshape(grid, length).astype(np.float32)


def spectral_tensor(rows, columns, length):
    wave_rows = 2.0 * math.pi / length * rows.astype(jnp.float32)
    wave_columns = 2.0 * math.pi / length * columns.astype(jnp.float32)
    squared = wave_rows * wave_rows + wave_columns * wave_columns
    nonzero = squared > 0.0
    safe = jnp.where(nonzero, squared, 1.0)
    scaled = jnp.sqrt(safe) * thickness
    film = jnp.where(nonzero, (1.0 - jnp.exp(-scaled)) / scaled, 1.0)
    in_plane = (1.0 - film) / safe
    half = length // 2
    edge_row = (rows == 0) | (rows == half)
    edge_column = (columns == 0) | (columns == half)
    weight = jnp.where(edge_row, 1.0, 2.0) * jnp.where(edge_column, 1.0, 2.0) * (-1.0 / (length * length))
    return (
        in_plane * wave_columns * wave_columns * weight,
        in_plane * wave_rows * wave_rows * weight,
        jnp.where(edge_row | edge_column, 0.0, in_plane * wave_columns * wave_rows * weight),
        film * weight,
    )


def exchange_field(padded, pad_coupling):
    center = padded[:, 1:-1]
    coupling = pad_coupling[1:-1]
    wide = jnp.pad(padded[:, 1:-1], ((0, 0), (0, 0), (1, 1)))
    wide_coupling = jnp.pad(coupling, ((0, 0), (1, 1)))
    total = pad_coupling[2:] * (padded[:, 2:] - center)
    total = total + pad_coupling[:-2] * (padded[:, :-2] - center)
    total = total + wide_coupling[:, 2:] * (wide[:, :, 2:] - center)
    total = total + wide_coupling[:, :-2] * (wide[:, :, :-2] - center)
    return stiffness * coupling * total


def cross(a, b):
    return jnp.stack([a[1] * b[2] - a[2] * b[1], a[2] * b[0] - a[0] * b[2], a[0] * b[1] - a[1] * b[0]])


def torque(magnet, effective):
    first = cross(magnet, effective)
    return -(first + damping * cross(magnet, first)) * (1.0 / (1.0 + damping * damping))


def coarse(padded, pad_coupling, field):
    center = padded[:, 1:-1]
    effective = exchange_field(padded, pad_coupling) + field
    effective = jnp.stack([effective[0], effective[1], effective[2] - center[2]])
    return center + FINE * step_time * torque(center, effective)


def dot(left, right):
    return jnp.dot(left, right, precision=lax.Precision.HIGH)


def halves(table):
    high = table.astype(jnp.bfloat16)
    return [high, (table - high.astype(np.float32)).astype(jnp.bfloat16)]


def split(value):
    high = value.astype(jnp.bfloat16)
    return high, (value - high.astype(jnp.float32)).astype(jnp.bfloat16)


def dot3(left_high, left_low, right_high, right_low):
    def one(a, b):
        return jnp.dot(a, b, preferred_element_type=jnp.float32)

    return one(left_high, right_high) + (one(left_high, right_low) + one(left_low, right_high))


def fine_kernel(
    space,
    start, field, links, coarse_end, tensors,
    cut_high, cut_low, up_high, up_low, tall_high, tall_low, back_high, back_low,
    out,
    current, rate, base, edge_out, edge_in, send, got, send_back, got_back,
    columns_high, columns_low, mixed_high, mixed_low, wide_high, wide_low, demag,
    edge_sems, send_sems, got_sems, send_back_sems, got_back_sems,
):
    _, rows, grid = start.shape
    rest = space // 2
    width = 2 * grid // space
    part = lax.axis_index("core") * rest + lax.axis_index("rest")

    def device(target):
        return {"core": target // rest, "rest": target % rest}

    barrier = pltpu.get_barrier_semaphore()

    def greet(k, carry):
        pl.semaphore_signal(
            barrier, inc=1, device_id=device((part + k) % space), device_id_type=pl.DeviceIdType.MESH
        )
        return carry

    lax.fori_loop(1, space, greet, 0)
    pl.semaphore_wait(barrier, space - 1)

    def remote(source, target, send_sem, recv_sem, where):
        return pltpu.make_async_remote_copy(
            src_ref=source, dst_ref=target, send_sem=send_sem, recv_sem=recv_sem,
            device_id=device(where), device_id_type=pl.DeviceIdType.MESH,
        )

    def forward(k):
        target = (part + k) % space
        return remote(send.at[target], got.at[part], send_sems.at[k], got_sems.at[k], target)

    def backward(k):
        target = (part + k) % space
        return remote(
            send_back.at[target], got_back.at[part], send_back_sems.at[k], got_back_sems.at[k], target
        )

    current[:, 8 : 8 + rows, :] = start[...]
    base[...] = start[...]

    def evaluate(parity):
        for c in range(3):
            edge_out[0, c : c + 1, :] = current[c, 8:9, :]
            edge_out[1, c : c + 1, :] = current[c, 7 + rows : 8 + rows, :]
        magnet_high, magnet_low = split(current[:, 8 : 8 + rows, :].reshape(3 * rows, grid))
        wide_high[:, :grid] = magnet_high
        wide_low[:, :grid] = magnet_low

        def block(index):
            return dot3(wide_high[:, :grid], wide_low[:, :grid], cut_high[index], cut_low[index])

        to_before = remote(
            edge_out.at[0], edge_in.at[parity, 1], edge_sems.at[0], edge_sems.at[1], (part + space - 1) % space
        )
        to_after = remote(
            edge_out.at[1], edge_in.at[parity, 0], edge_sems.at[2], edge_sems.at[3], (part + 1) % space
        )
        to_before.start()
        to_after.start()

        def push(k, carry):
            target = (part + k) % space
            send[target] = block(target)
            forward(k).start()
            return carry

        lax.fori_loop(1, space, push, 0)
        got[part] = block(part)

        def take(k, carry):
            forward(k).wait()
            return carry

        lax.fori_loop(1, space, take, 0)
        to_before.wait()
        to_after.wait()
        for c in range(3):
            current[c, 7:8, :] = edge_in[parity, 0, c : c + 1, :]
            current[c, 8 + rows : 9 + rows, :] = edge_in[parity, 1, c : c + 1, :]
        columns = jnp.concatenate(
            [got[:, c * rows : (c + 1) * rows, :].reshape(grid, width) for c in range(3)], axis=1
        )
        columns_high[...], columns_low[...] = split(columns)

        step = grid // 2

        def mix(i, carry):
            lower = pl.multiple_of(i * step, step)
            upper = pl.multiple_of(grid + i * step, step)

            def spectrum(at):
                return dot3(
                    up_high[pl.ds(at, step), :], up_low[pl.ds(at, step), :], columns_high[...], columns_low[...]
                )

            pair = (spectrum(lower), spectrum(upper))
            for q, at in enumerate((lower, upper)):
                txx, tyy, txy, tzz = (tensors[n, pl.ds(at, step), :] for n in range(4))
                sx, sy, sz = (pair[q][:, c * width : (c + 1) * width] for c in range(3))
                ox, oy = (pltpu.roll(pair[1 - q][:, c * width : (c + 1) * width], width // 2, 1) for c in range(2))
                for c, value in enumerate((txx * sx + txy * oy, txy * ox + tyy * sy, tzz * sz)):
                    high, low = split(value)
                    mixed_high[pl.ds(at, step), c * width : (c + 1) * width] = high
                    mixed_low[pl.ds(at, step), c * width : (c + 1) * width] = low
            return carry

        lax.fori_loop(0, 2, mix, 0)

        def synth(i, carry):
            at = pl.multiple_of(i * step, step)
            value = dot3(
                tall_high[pl.ds(at, step), :], tall_low[pl.ds(at, step), :], mixed_high[...], mixed_low[...]
            )
            send_back[pl.ds(i * (space // 2), space // 2)] = value.reshape(space // 2, rows, 3 * width)

            def push_back(j, inner):
                target = i * (space // 2) + j

                @pl.when(target != part)
                def _():
                    backward((target - part + space) % space).start()

                return inner

            return lax.fori_loop(0, space // 2, push_back, carry)

        lax.fori_loop(0, 2, synth, 0)

        got_back[part] = send_back[part]

        def take_back(k, carry):
            backward(k).wait()
            return carry

        lax.fori_loop(1, space, take_back, 0)
        for j in range(space):
            for c in range(3):
                high, low = split(got_back[j, :, c * width : (c + 1) * width])
                wide_high[c * rows : (c + 1) * rows, j * width : (j + 1) * width] = high
                wide_low[c * rows : (c + 1) * rows, j * width : (j + 1) * width] = low
        demag[...] = dot3(wide_high[...], wide_low[...], back_high[...], back_low[...])

        for at in range(0, rows, 8):
            inside = [current[c, 8 + at : 16 + at, :] for c in range(3)]
            weights = [links[n, at : at + 8, :] for n in range(4)]
            effective = []
            for c in range(3):
                m = inside[c]
                total = weights[0] * (current[c, 7 + at : 15 + at, :] - m)
                total = total + weights[1] * (current[c, 9 + at : 17 + at, :] - m)
                total = total + weights[2] * (pltpu.roll(m, 1, 1) - m)
                total = total + weights[3] * (pltpu.roll(m, grid - 1, 1) - m)
                effective.append(total + demag[c * rows + at : c * rows + at + 8, :] + field[c, at : at + 8, :])
            first = cross_of(inside, effective)
            second = cross_of(inside, first)
            for c in range(3):
                value = -(first[c] + damping * second[c]) * (1.0 / (1.0 + damping * damping))
                if parity == 0:
                    rate[c, at : at + 8, :] = value
                else:
                    moved = base[c, at : at + 8, :] + 0.5 * step_time * (rate[c, at : at + 8, :] + value)
                    base[c, at : at + 8, :] = moved
        if parity == 0:
            current[:, 8 : 8 + rows, :] = base[...] + step_time * rate[...]
        else:
            current[:, 8 : 8 + rows, :] = base[...]

    def fine_step(i, carry):
        evaluate(0)
        evaluate(1)
        return carry

    lax.fori_loop(0, FINE, fine_step, 0)
    out[...] = base[...] - coarse_end[...]


def cross_of(a, b):
    return [a[1] * b[2] - a[2] * b[1], a[2] * b[0] - a[0] * b[2], a[0] * b[1] - a[1] * b[0]]


def fine_jump(space, start, field, links, coarse_end, tensors, tables):
    _, rows, grid = start.shape
    length = 2 * grid
    width = length // space

    def kernel(*refs):
        fine_kernel(space, *refs)

    f32, bf16 = jnp.float32, jnp.bfloat16
    operands = [start, field, links, coarse_end, tensors, *tables]
    return pl.pallas_call(
        kernel,
        out_shape=jax.ShapeDtypeStruct(start.shape, f32),
        in_specs=[pl.BlockSpec(memory_space=pltpu.VMEM)] * len(operands),
        out_specs=pl.BlockSpec(memory_space=pltpu.VMEM),
        scratch_shapes=[
            pltpu.VMEM((3, rows + 16, grid), f32),
            pltpu.VMEM((3, rows, grid), f32),
            pltpu.VMEM((3, rows, grid), f32),
            pltpu.VMEM((2, 8, grid), f32),
            pltpu.VMEM((2, 2, 8, grid), f32),
            pltpu.VMEM((space, 3 * rows, width), f32),
            pltpu.VMEM((space, 3 * rows, width), f32),
            pltpu.VMEM((space, rows, 3 * width), f32),
            pltpu.VMEM((space, rows, 3 * width), f32),
            pltpu.VMEM((grid, 3 * width), bf16),
            pltpu.VMEM((grid, 3 * width), bf16),
            pltpu.VMEM((length, 3 * width), bf16),
            pltpu.VMEM((length, 3 * width), bf16),
            pltpu.VMEM((3 * rows, length), bf16),
            pltpu.VMEM((3 * rows, length), bf16),
            pltpu.VMEM((3 * rows, grid), f32),
            pltpu.SemaphoreType.DMA((4,)),
            pltpu.SemaphoreType.DMA((space,)),
            pltpu.SemaphoreType.DMA((space,)),
            pltpu.SemaphoreType.DMA((space,)),
            pltpu.SemaphoreType.DMA((space,)),
        ],
        compiler_params=pltpu.CompilerParams(
            collective_id=0, has_side_effects=True, vmem_limit_bytes=56 * 1024 * 1024
        ),
    )(*operands)


def links_of(pad_coupling, depth):
    rows = pad_coupling.shape[0] - 2 * depth
    own = pad_coupling[depth : rows + depth]
    flat = jnp.pad(own, ((0, 0), (1, 1)))
    around = [
        pad_coupling[depth - 1 : rows + depth - 1],
        pad_coupling[depth + 1 : rows + depth + 1],
        flat[:, :-2],
        flat[:, 2:],
    ]
    return stiffness * own[None] * jnp.stack(around)


def sweep_kernel(
    space, tm, jump, opening, field, links, out,
    current, landed, edge_out, edge_in, swap_sems, send_sems, recv_sems,
):
    _, rows, grid = opening.shape
    rest = space // 2
    core, zh = lax.axis_index("core"), lax.axis_index("zh")
    number = lax.axis_index("x") * 2 + core
    place = zh * rest + lax.axis_index("rest")
    mesh_type = pl.DeviceIdType.MESH

    def device(slice_number, target):
        target = (target + space) % space
        return {
            "x": slice_number // 2, "core": slice_number % 2, "zh": target // rest, "rest": target % rest,
        }

    crossing = core != zh
    later, earlier = number < tm - 1, number > 0
    barrier = pltpu.get_barrier_semaphore()
    partner = {"core": zh, "zh": core}

    def greet(where):
        pl.semaphore_signal(barrier, inc=1, device_id=where, device_id_type=mesh_type)

    @pl.when(crossing)
    def _():
        greet(partner)

    @pl.when(later)
    def _():
        for shift in (-1, 0, 1):
            greet(device(number + 1, place + shift))

    @pl.when(earlier)
    def _():
        for shift in (-1, 0, 1):
            greet(device(number - 1, place + shift))

    amount = jnp.where(crossing, 1, 0) + jnp.where(later, 3, 0) + jnp.where(earlier, 3, 0)
    pl.semaphore_wait(barrier, amount)

    swap = pltpu.make_async_remote_copy(
        src_ref=jump, dst_ref=landed, send_sem=swap_sems.at[0], recv_sem=swap_sems.at[1],
        device_id=partner, device_id_type=mesh_type,
    )

    @pl.when(crossing)
    def _():
        swap.start()

    def outgoing():
        target = number + 1

        def one(n, source, landing, shift):
            return pltpu.make_async_remote_copy(
                src_ref=source, dst_ref=landing, send_sem=send_sems.at[n], recv_sem=recv_sems.at[n],
                device_id=device(target, place + shift), device_id_type=mesh_type,
            )

        return [
            one(0, out, current.at[:, 8 : 8 + rows, :], 0),
            one(1, edge_out.at[0], edge_in.at[1], -1),
            one(2, edge_out.at[1], edge_in.at[0], 1),
        ]

    @pl.when(crossing)
    def _():
        swap.wait()

    @pl.when(core == zh)
    def _():
        landed[...] = jump[...]

    @pl.when(number == 0)
    def _():
        out[...] = opening[...] + landed[...]

    @pl.when(earlier)
    def _():
        for copy in outgoing():
            copy.wait_recv()
        for c in range(3):
            current[c, 7:8, :] = edge_in[0, c : c + 1, :]
            current[c, 8 + rows : 9 + rows, :] = edge_in[1, c : c + 1, :]
        for at in range(0, rows, 8):
            inside = [current[c, 8 + at : 16 + at, :] for c in range(3)]
            weights = [links[n, at : at + 8, :] for n in range(4)]
            effective = []
            for c in range(3):
                m = inside[c]
                total = weights[0] * (current[c, 7 + at : 15 + at, :] - m)
                total = total + weights[1] * (current[c, 9 + at : 17 + at, :] - m)
                total = total + weights[2] * (pltpu.roll(m, 1, 1) - m)
                total = total + weights[3] * (pltpu.roll(m, grid - 1, 1) - m)
                total = total + field[c, at : at + 8, :]
                effective.append(total - m if c == 2 else total)
            first = cross_of(inside, effective)
            second = cross_of(inside, first)
            for c in range(3):
                value = -(first[c] + damping * second[c]) * (1.0 / (1.0 + damping * damping))
                moved = inside[c] + FINE * step_time * value
                out[c, at : at + 8, :] = moved + landed[c, at : at + 8, :]

    @pl.when(later)
    def _():
        for c in range(3):
            edge_out[0, c : c + 1, :] = out[c, 0:1, :]
            edge_out[1, c : c + 1, :] = out[c, rows - 1 : rows, :]
        copies = outgoing()
        for copy in copies:
            copy.start()
        for copy in copies:
            copy.wait_send()


def sweep(space, tm, jump, opening, field, links):
    _, rows, grid = opening.shape
    f32 = jnp.float32

    def kernel(*refs):
        sweep_kernel(space, tm, *refs)

    return pl.pallas_call(
        kernel,
        out_shape=jax.ShapeDtypeStruct(opening.shape, f32),
        in_specs=[pl.BlockSpec(memory_space=pltpu.VMEM)] * 4,
        out_specs=pl.BlockSpec(memory_space=pltpu.VMEM),
        scratch_shapes=[
            pltpu.VMEM((3, rows + 16, grid), f32),
            pltpu.VMEM((3, rows, grid), f32),
            pltpu.VMEM((2, 8, grid), f32),
            pltpu.VMEM((2, 8, grid), f32),
            pltpu.SemaphoreType.DMA((2,)),
            pltpu.SemaphoreType.DMA((3,)),
            pltpu.SemaphoreType.DMA((3,)),
        ],
        compiler_params=pltpu.CompilerParams(
            collective_id=1, has_side_effects=True, vmem_limit_bytes=32 * 1024 * 1024
        ),
    )(jump, opening, field, links)


def make_shards(tm, space):
    rest = space // 2

    def shards(initial_state, applied_field, coupling):
        rows, _, grid = initial_state.shape
        length = 2 * grid
        width = length // space
        depth = tm
        part = lax.axis_index(RING)
        new_slice = lax.axis_index(("x", "zh"))
        tall, blocks = real_tables(grid, space)

        start = jnp.transpose(initial_state, (1, 0, 2))
        field = jnp.transpose(applied_field, (1, 0, 2))
        pack = jnp.concatenate([start, field, coupling[None]], axis=0)

        def fetch(block, shift):
            pairs = []
            for device in range(2 * space):
                core, zh, r = device // space, device // rest % 2, device % rest
                wanted = core * rest + r + shift
                if 0 <= wanted < space:
                    pairs.append((zh * space + wanted, device))
            return lax.ppermute(block, LOCAL, pairs)

        middle = fetch(pack, 0)
        before = fetch(pack[:, rows - depth :], -1)
        after = fetch(pack[:, :depth], 1)
        wide = jnp.concatenate([before, middle, after], axis=1)
        wide_coupling = wide[6]
        wide_field = wide[3:6]
        state = wide[:3]
        fine_start, coarse_end = state, state
        for n in range(tm):
            stepped = jnp.pad(
                coarse(state, wide_coupling, wide_field[:, 1:-1]), ((0, 0), (1, 1), (0, 0))
            )
            here = new_slice == n
            fine_start = jnp.where(here, state, fine_start)
            coarse_end = jnp.where(here, stepped, coarse_end)
            state = stepped
        fine_field = wide_field[:, depth:-depth]
        fine_coupling = wide_coupling[depth - 1 : rows + depth + 1]
        coarse_end = coarse_end[:, depth:-depth]

        slot = jnp.arange(length, dtype=jnp.int32)
        wave_y = jnp.where(slot == grid, grid, slot % grid)
        lane = jnp.arange(width, dtype=jnp.int32)
        wave_x = part * (width // 2) + lane % (width // 2)
        wave_x = jnp.where((wave_x == 0) & (lane >= width // 2), grid, wave_x)
        txx, tyy, txy, tzz = spectral_tensor(wave_y[:, None], wave_x[None, :], length)
        same = ((slot >= grid)[:, None]) == ((lane >= width // 2)[None, :])
        txy = jnp.where(same, -txy, txy)

        links = links_of(wide_coupling, depth)
        cut = np.transpose(blocks.reshape(grid, space, width), (1, 0, 2))
        tables = [part_ for table in (cut, tall.T, tall, blocks.T) for part_ in halves(table)]
        jump = fine_jump(
            space, fine_start[:, depth:-depth], fine_field, links, coarse_end, jnp.stack([txx, tyy, txy, tzz]), tables
        )
        def beside(block, shift):
            pairs = [(i - shift, i) for i in range(space) if 0 <= i - shift < space]
            return lax.ppermute(block, ("zh", "rest"), pairs)

        packed = jnp.concatenate([start, coupling[None]], axis=0)
        home = jnp.concatenate([beside(packed[:, -1:], 1), packed, beside(packed[:, :1], -1)], axis=1)
        home_coupling = home[3]
        opening = coarse(home[:3], home_coupling, field)
        end = sweep(space, tm, jump, opening, field, links_of(home_coupling, 1))
        return jnp.transpose(end, (1, 0, 2))[None]

    return shards


def solution(mesh):
    tm, space = mesh.shape["tm"], mesh.shape["space"]
    finer = Mesh(mesh.devices.reshape(tm // 2, 2, 2, space // 2), EVERY)
    rows = ("zh", "rest")
    return jax.shard_map(
        make_shards(tm, space),
        mesh=finer,
        in_specs=(P(rows, None, None), P(rows, None, None), P(rows, None)),
        out_specs=P(("x", "core"), rows, None, None),
        check_vma=False,
    )
```
